32 devices in a mesh: row: 4 (over z), col: 8 (over y, x, core).
Axes of the slice: x: 2, y: 2, z: 4, core: 2. Of those that a mesh axis runs over, the one named last changes fastest.
Arguments:
- right_side: float32 [256, 2048], P('row', 'col'), may hold values from -20 to 20
- initial_guess: float32 [256, 2048], P('row', 'col'), may hold values from -3 to 3
- kernel: float32 [31, 31], replicated, may hold values from 0 to 1, as said below
Outputs:
- template: float32 [256, 2048], P('row', 'col')
- residual: float32 [256, 2048], P('row', 'col')
The draws below stay inside these ranges and needn't reach their ends.
Inputs may be any that keep to these rules, and one draw needn't show every extreme that they name: `kernel`: entries are positive and sum to one.
All inputs are finite; a program needn't handle non-finite values.
Results may differ from the reference program's by a relative error of at most 0.0003.
Values sent between devices are 32-bit elements; how exact they have to be, the bound alone decides.
A program may use at most 128 MiB of HBM per device.

```python
import jax
import jax.numpy as jnp

KW = 31
ITERS = 3
NX = 256
NY = 2048


def draw_right_side(key, part):
    rough = jax.random.normal(jax.random.fold_in(key, 11), (NX, NY), jnp.float32)
    column_pos = jnp.arange(NY, dtype=jnp.float32) / max(NY - 1, 1)
    ramp = jnp.exp(jnp.log(3.0) * column_pos)[None, :]
    values = rough * ramp
    return jnp.clip(values, -20.0, 20.0)


def draw_kernel(key, part):
    center = (KW - 1) / 2.0
    offsets = jnp.arange(KW, dtype=jnp.float32) - center
    radius_sq = offsets[:, None] ** 2 + offsets[None, :] ** 2
    profile = jnp.exp(-radius_sq / 98.0)
    factor = jax.random.uniform(jax.random.fold_in(key, 21), (KW, KW), jnp.float32, 0.5, 1.5)
    weights = profile * factor
    return weights / jnp.sum(weights)


def shard_levels(own_key, shape, shards, least, largest):
    def one(position, blocks):
        draws = jax.random.uniform(jax.random.fold_in(jax.random.fold_in(own_key, 6), position), (blocks,), jnp.float32, least / len(shards), largest / len(shards))
        return jnp.repeat(jnp.exp(draws), shape[position] // blocks).reshape((-1,) + (1,) * (len(shape) - position - 1))

    gain = one(*shards[0])
    for cut in shards[1:]:
        gain = gain * one(*cut)
    return gain


def scatter_about(rng, dims, deviation, bound, split=(), kind=jnp.bfloat16):
    level = shard_levels(rng, dims, split, -0.22, 0.18) if split else 1.0
    result = jax.random.normal(rng, dims, jnp.float32) * deviation * level
    return jnp.minimum(jnp.maximum(result, -bound), bound).astype(kind)


def setup_inputs(seed: int = 0) -> dict:
    splits = jax.random.split(jax.random.key(seed), 4)
    return {
        "right_side": draw_right_side(jax.random.fold_in(splits[3], 71), 0),
        "initial_guess": scatter_about(splits[1], (NX, NY), 0.5, 3.0, ((0, 4), (1, 8)), jnp.float32),
        "kernel": draw_kernel(jax.random.fold_in(splits[3], 71), 0),
    }


penalty = 0.05


def convolve(source, taps):
    half_width = taps.shape[0] // 2
    tile_rows, tile_cols = source.shape
    extent = (tile_rows + 2 * half_width, tile_cols + 2 * half_width)
    spectrum = jnp.fft.rfft2(source, s=extent) * jnp.fft.rfft2(taps, s=extent)
    complete = jnp.fft.irfft2(spectrum, s=extent)
    return complete[half_width:half_width + tile_rows, half_width:half_width + tile_cols].astype(source.dtype)


def laplacian(source):
    padded = jnp.pad(source, 1)
    return 4.0 * source - padded[2:, 1:-1] - padded[:-2, 1:-1] - padded[1:-1, 2:] - padded[1:-1, :-2]


def operate(source, kernel):
    blurred = convolve(source, kernel[::-1, ::-1])
    return convolve(blurred, kernel) + penalty * laplacian(source)


def reference(right_side, initial_guess, kernel):
    template = initial_guess
    residual = right_side - operate(template, kernel)
    direction = residual
    norm_now = jnp.sum(residual * residual)
    for iteration in range(ITERS):
        applied = operate(direction, kernel)
        step_size = norm_now / jnp.sum(direction * applied)
        template = template + step_size * direction
        residual = residual - step_size * applied
        norm_next = jnp.sum(residual * residual)
        direction = residual + (norm_next / norm_now) * direction
        norm_now = norm_next
    return template, residual
```

```python
import functools

import jax
import jax.numpy as jnp
from jax import lax
from jax.experimental import pallas as pl
from jax.experimental.pallas import tpu as pltpu
from jax.sharding import PartitionSpec as P

ITERS = 3
PENALTY = 0.05
EDGE_ROWS = 16
EDGE_COLS = 128
GROUP = 8
MESH = pl.DeviceIdType.MESH
DIRECTIONS = ((-1, -1), (-1, 1), (1, -1), (1, 1), (-1, 0), (1, 0), (0, -1), (0, 1))


def span(step, size, edge):
    if step > 0:
        return size, 0, edge
    if step < 0:
        return edge, size + edge, edge
    return edge, edge, size


def split(x):
    high = x.astype(jnp.bfloat16)
    low = (x - high.astype(jnp.float32)).astype(jnp.bfloat16)
    return high, low


def body(
    n_row, n_col, half,
    right_ref, guess_ref, base_ref, template_ref, residual_ref,
    ext, tables, red, send_sem, recv_sem, red_send, red_recv,
):
    rows, cols = right_ref.shape
    row, col = lax.axis_index("row"), lax.axis_index("col")
    me, count = row * n_col + col, n_row * n_col
    tall, wide = rows + 2 * EDGE_ROWS, cols + 2 * EDGE_COLS
    groups = tables.shape[1]
    mid_r, mid_c = pl.ds(EDGE_ROWS, rows), pl.ds(EDGE_COLS, cols)

    barrier = pltpu.get_barrier_semaphore()

    def greet(step, carry):
        other = lax.rem(me + step, count)
        pl.semaphore_signal(
            barrier, inc=1, device_id=(other // n_col, lax.rem(other, n_col)), device_id_type=MESH
        )
        return carry

    lax.fori_loop(1, count, greet, 0)

    phases = ext.shape[0]
    ext[0, mid_r, mid_c] = guess_ref[...]

    @pl.when(row == 0)
    def _():
        ext[:, 0:EDGE_ROWS, :] = jnp.zeros((phases, EDGE_ROWS, wide), jnp.float32)

    @pl.when(row == n_row - 1)
    def _():
        ext[:, EDGE_ROWS + rows : tall, :] = jnp.zeros((phases, EDGE_ROWS, wide), jnp.float32)

    @pl.when(col == 0)
    def _():
        ext[:, :, 0:EDGE_COLS] = jnp.zeros((phases, tall, EDGE_COLS), jnp.float32)

    @pl.when(col == n_col - 1)
    def _():
        ext[:, :, EDGE_COLS + cols : wide] = jnp.zeros((phases, tall, EDGE_COLS), jnp.float32)

    def inside(dr, dc):
        checks = []
        if dr:
            checks.append(row + dr >= 0 if dr < 0 else row + dr < n_row)
        if dc:
            checks.append(col + dc >= 0 if dc < 0 else col + dc < n_col)
        return functools.reduce(jnp.logical_and, checks)

    def strip(phase, index):
        dr, dc = DIRECTIONS[index]
        r_src, r_dst, r_len = span(dr, rows, EDGE_ROWS)
        c_src, c_dst, c_len = span(dc, cols, EDGE_COLS)
        return pltpu.make_async_remote_copy(
            src_ref=ext.at[phase, pl.ds(r_src, r_len), pl.ds(c_src, c_len)],
            dst_ref=ext.at[phase, pl.ds(r_dst, r_len), pl.ds(c_dst, c_len)],
            send_sem=send_sem.at[phase, index],
            recv_sem=recv_sem.at[phase, index],
            device_id=(row + dr, col + dc),
            device_id_type=MESH,
        )

    def send(phase):
        for index, (dr, dc) in enumerate(DIRECTIONS):
            pl.when(inside(dr, dc))(lambda index=index: strip(phase, index).start())

    def receive(phase):
        for index, (dr, dc) in enumerate(DIRECTIONS):
            pl.when(inside(-dr, -dc))(lambda index=index: strip(phase, index).wait_recv())

    def finish(phase):
        for index, (dr, dc) in enumerate(DIRECTIONS):
            pl.when(inside(dr, dc))(lambda index=index: strip(phase, index).wait_send())

    sub = lax.broadcasted_iota(jnp.int32, (8, base_ref.shape[2]), 0)

    def build(which):
        for group in range(groups):
            line = base_ref[which, group : group + 1, :]
            eight = pltpu.roll(
                jnp.broadcast_to(line, (8, line.shape[1])), EDGE_ROWS - half, axis=1
            )
            for bit in (1, 2, 4):
                eight = jnp.where((sub & bit) != 0, pltpu.roll(eight, bit, axis=1), eight)
            blocks = [eight if k == 0 else pltpu.roll(eight, 8 * k, axis=1) for k in range(rows // 8)]
            high, low = split(jnp.concatenate(blocks, axis=0))
            tables[which, group, 0:rows, :] = high
            tables[which, group, rows : 2 * rows, :] = low

    def correlate(phase, which):
        both = jnp.zeros((2 * rows, cols), jnp.float32)
        rest = jnp.zeros((rows, cols), jnp.float32)
        whole = ext[phase]
        for group in range(groups):
            highs, lows = [], []
            for k in range(GROUP):
                offset = EDGE_COLS - half + group * GROUP + k
                high, low = split(pltpu.roll(whole, wide - offset, axis=1)[:, 0:cols])
                highs.append(high)
                lows.append(low)
            table = tables[which, group]
            both = both + jnp.dot(
                table, jnp.concatenate(highs, axis=0), preferred_element_type=jnp.float32
            )
            rest = rest + jnp.dot(
                table[0:rows], jnp.concatenate(lows, axis=0), preferred_element_type=jnp.float32
            )
        return both[0:rows] + (both[rows:] + rest)

    def laplacian(phase):
        center = ext[phase, mid_r, mid_c]
        upper = ext[phase, pl.ds(EDGE_ROWS - 1, rows), mid_c]
        lower = ext[phase, pl.ds(EDGE_ROWS + 1, rows), mid_c]
        band = ext[phase, mid_r, :]
        left = pltpu.roll(band, 1, axis=1)[:, EDGE_COLS : EDGE_COLS + cols]
        right = pltpu.roll(band, wide - 1, axis=1)[:, EDGE_COLS : EDGE_COLS + cols]
        return 4.0 * center - upper - lower - left - right

    def operate(phase):
        receive(phase)
        ext[phase + 1, mid_r, mid_c] = correlate(phase, 0)
        send(phase + 1)
        smooth = PENALTY * laplacian(phase)
        receive(phase + 1)
        return correlate(phase + 1, 1) + smooth

    def put(phase, value):
        ext[phase, mid_r, mid_c] = value
        send(phase)

    lane = lax.broadcasted_iota(jnp.int32, (1, 128), 1)

    def fold(x):
        line = jnp.sum(x, axis=0, keepdims=True)
        line = functools.reduce(
            jnp.add, [line[:, k : k + 128] for k in range(0, line.shape[1], 128)]
        )
        return line + pltpu.roll(line, 64, axis=1)

    def spread(slot, residual, applied):
        red[slot, me] = jnp.where(lane < 64, fold(residual * residual), fold(residual * applied))

        def one(step, carry):
            other = lax.rem(me + step, count)
            pltpu.make_async_remote_copy(
                src_ref=red.at[slot, me],
                dst_ref=red.at[slot, me],
                send_sem=red_send.at[slot],
                recv_sem=red_recv.at[slot],
                device_id=(other // n_col, lax.rem(other, n_col)),
                device_id_type=MESH,
            ).start()
            return carry

        lax.fori_loop(1, count, one, 0)

    def all_slots(slot):
        return pltpu.make_async_remote_copy(
            src_ref=red.at[slot, pl.ds(0, count - 1)],
            dst_ref=red.at[slot, pl.ds(0, count - 1)],
            send_sem=red_send.at[slot],
            recv_sem=red_recv.at[slot],
            device_id=(row, col),
            device_id_type=MESH,
        )

    def gather(slot):
        all_slots(slot).wait_recv()
        line = jnp.sum(red[slot], axis=0)
        norm = jnp.sum(jnp.where(lane < 64, line, 0.0), axis=1, keepdims=True)
        product = jnp.sum(jnp.where(lane < 64, 0.0, line), axis=1, keepdims=True)
        return norm, product

    pl.semaphore_wait(barrier, count - 1)
    send(0)
    build(0)
    build(1)

    template = guess_ref[...]
    residual = right_ref[...] - operate(0)
    put(2, residual)
    applied = operate(2)
    norm_last = step_size = None
    direction = along = beyond = None
    for iteration in range(ITERS):
        last = iteration + 1 == ITERS
        if not last:
            put(4 + 2 * iteration, applied)
        spread(iteration, residual, applied)
        twice = None if last else operate(4 + 2 * iteration)
        norm, product = gather(iteration)
        if iteration == 0:
            step_size = norm / product
            direction, along, beyond = residual, applied, twice
        else:
            ratio = norm / norm_last
            step_size = norm / (product - ratio * norm / step_size)
            direction = residual + ratio * direction
            along = applied + ratio * along
            if not last:
                beyond = twice + ratio * beyond
        norm_last = norm
        template = template + step_size * direction
        residual = residual - step_size * along
        if not last:
            applied = applied - step_size * beyond

    template_ref[...] = template
    residual_ref[...] = residual
    for phase in range(phases):
        finish(phase)
    for slot in range(ITERS):
        all_slots(slot).wait_send()


def on_device(n_row, n_col, right_side, initial_guess, kernel):
    rows, cols = right_side.shape
    width = kernel.shape[0]
    tall = rows + 2 * EDGE_ROWS
    groups = -(-width // GROUP)
    both = jnp.stack([kernel.T, kernel[::-1, ::-1].T])
    base = jnp.pad(both, ((0, 0), (0, groups * GROUP - width), (0, tall - width)))
    base = base.reshape(2, groups, GROUP * tall)
    phases, count = 2 * (ITERS + 1), n_row * n_col
    shape = jax.ShapeDtypeStruct((rows, cols), jnp.float32)
    vmem = pl.BlockSpec(memory_space=pltpu.VMEM)
    return pl.pallas_call(
        functools.partial(body, n_row, n_col, width // 2),
        out_shape=(shape, shape),
        in_specs=[vmem] * 3,
        out_specs=(vmem, vmem),
        scratch_shapes=[
            pltpu.VMEM((phases, tall, cols + 2 * EDGE_COLS), jnp.float32),
            pltpu.VMEM((2, groups, 2 * rows, GROUP * tall), jnp.bfloat16),
            pltpu.VMEM((ITERS, count, 1, 128), jnp.float32),
            pltpu.SemaphoreType.DMA((phases, len(DIRECTIONS))),
            pltpu.SemaphoreType.DMA((phases, len(DIRECTIONS))),
            pltpu.SemaphoreType.DMA((ITERS,)),
            pltpu.SemaphoreType.DMA((ITERS,)),
        ],
        compiler_params=pltpu.CompilerParams(collective_id=0, has_side_effects=True),
    )(right_side, initial_guess, base)


def solution(mesh):
    placed = (P("row", "col"), P("row", "col"), P())
    return jax.shard_map(
        functools.partial(on_device, mesh.shape["row"], mesh.shape["col"]),
        mesh=mesh,
        in_specs=placed,
        out_specs=(P("row", "col"), P("row", "col")),
        check_vma=False,
    )
```

```python
import functools

import jax
import jax.numpy as jnp
from jax import lax
from jax.experimental import pallas as pl
from jax.experimental.pallas import tpu as pltpu
from jax.sharding import PartitionSpec as P

ITERS = 3
PENALTY = 0.05
EDGE_ROWS = 16
EDGE_COLS = 128
DEPTH = 512
LANES = 128
MESH = pl.DeviceIdType.MESH
DIRECTIONS = ((-1, -1), (-1, 1), (1, -1), (1, 1), (0, -1), (0, 1), (-1, 0), (1, 0))
SIDES = (4, 5)
OTHERS = (0, 1, 2, 3, 6, 7)


def span(step, size, edge):
    if step > 0:
        return size, 0, edge
    if step < 0:
        return edge, size + edge, edge
    return edge, edge, size


def split(x):
    high = x.astype(jnp.bfloat16)
    low = (x - high.astype(jnp.float32)).astype(jnp.bfloat16)
    return high, low


def body(
    n_row, n_col,
    right_ref, guess_ref, kernel_ref, template_ref, residual_ref,
    ext, mid_table, edge_table, red, send_sem, recv_sem, red_send, red_recv,
):
    rows, cols = right_ref.shape
    row, col = lax.axis_index("row"), lax.axis_index("col")
    me, count = row * n_col + col, n_row * n_col
    tall, wide = rows + 2 * EDGE_ROWS, cols + 2 * EDGE_COLS
    width = kernel_ref.shape[0]
    half = width // 2
    shifts = mid_table.shape[2] // rows
    mid_r, mid_c = pl.ds(EDGE_ROWS, rows), pl.ds(EDGE_COLS, cols)

    barrier = pltpu.get_barrier_semaphore()

    def others(act):
        def along_row(r, carry):
            def one(c, inner):
                pl.when(r * n_col + c != me)(lambda: act((r, c)))
                return inner

            return lax.fori_loop(0, n_col, one, carry)

        lax.fori_loop(0, n_row, along_row, 0)

    others(
        lambda place: pl.semaphore_signal(barrier, inc=1, device_id=place, device_id_type=MESH)
    )

    phases = ext.shape[0]
    ext[0, mid_r, mid_c] = guess_ref[...]

    @pl.when(row == 0)
    def _():
        ext[:, 0:EDGE_ROWS, :] = jnp.zeros((phases, EDGE_ROWS, wide), jnp.float32)

    @pl.when(row == n_row - 1)
    def _():
        ext[:, EDGE_ROWS + rows : tall, :] = jnp.zeros((phases, EDGE_ROWS, wide), jnp.float32)

    @pl.when(col == 0)
    def _():
        ext[:, :, 0:EDGE_COLS] = jnp.zeros((phases, tall, EDGE_COLS), jnp.float32)

    @pl.when(col == n_col - 1)
    def _():
        ext[:, :, EDGE_COLS + cols : wide] = jnp.zeros((phases, tall, EDGE_COLS), jnp.float32)

    def inside(dr, dc):
        checks = []
        if dr:
            checks.append(row + dr >= 0 if dr < 0 else row + dr < n_row)
        if dc:
            checks.append(col + dc >= 0 if dc < 0 else col + dc < n_col)
        return functools.reduce(jnp.logical_and, checks)

    def strip(phase, index):
        dr, dc = DIRECTIONS[index]
        r_src, r_dst, r_len = span(dr, rows, EDGE_ROWS)
        c_src, c_dst, c_len = span(dc, cols, EDGE_COLS)
        return pltpu.make_async_remote_copy(
            src_ref=ext.at[phase, pl.ds(r_src, r_len), pl.ds(c_src, c_len)],
            dst_ref=ext.at[phase, pl.ds(r_dst, r_len), pl.ds(c_dst, c_len)],
            send_sem=send_sem.at[phase, index],
            recv_sem=recv_sem.at[phase, index],
            device_id=(row + dr, col + dc),
            device_id_type=MESH,
        )

    def send(phase):
        for index, (dr, dc) in enumerate(DIRECTIONS):
            pl.when(inside(dr, dc))(lambda index=index: strip(phase, index).start())

    def receive(phase, which):
        for index in which:
            dr, dc = DIRECTIONS[index]
            pl.when(inside(-dr, -dc))(lambda index=index: strip(phase, index).wait_recv())

    def finish(phase):
        for index, (dr, dc) in enumerate(DIRECTIONS):
            pl.when(inside(dr, dc))(lambda index=index: strip(phase, index).wait_send())

    sub = lax.broadcasted_iota(jnp.int32, (8, LANES), 0)
    lane8 = lax.broadcasted_iota(jnp.int32, (8, LANES), 1)
    per_mid, edge_span = LANES // rows, 2 * EDGE_ROWS
    per_edge = LANES // edge_span

    def build(which):
        taps = kernel_ref[...]
        if which:
            taps = jnp.concatenate([taps[a : a + 1] for a in reversed(range(width))], axis=0)
        taps = jnp.concatenate([taps, jnp.zeros((LANES - width, width), jnp.float32)], axis=0)
        taps = jnp.concatenate([taps, jnp.zeros((LANES, LANES - width), jnp.float32)], axis=1)
        taps = taps.T
        bands = []
        for b in range(shifts):
            if b >= width:
                bands.append(None)
                continue
            source = width - 1 - b if which else b
            eight = pltpu.roll(
                jnp.broadcast_to(taps[source : source + 1, :], (8, LANES)), EDGE_ROWS - half, axis=1
            )
            for bit in (1, 2, 4):
                eight = jnp.where((sub & bit) != 0, pltpu.roll(eight, bit, axis=1), eight)
            bands.append(eight)

        def moved(b, k, shift):
            if bands[b] is None:
                return jnp.zeros((8, LANES), jnp.float32)
            return pltpu.roll(bands[b], (8 * k + shift) % LANES, axis=1)

        def keep(table, tile, blocks):
            high, low = split(jnp.concatenate(blocks, axis=0))
            table[which, 0:rows, tile * LANES : (tile + 1) * LANES] = high
            table[which, rows : 2 * rows, tile * LANES : (tile + 1) * LANES] = low

        for tile in range(shifts // per_mid):
            blocks = []
            for k in range(rows // 8):
                block = moved(tile * per_mid, k, -EDGE_ROWS)
                for q in range(1, per_mid):
                    block = jnp.where(
                        lane8 < q * rows,
                        block,
                        moved(tile * per_mid + q, k, q * rows - EDGE_ROWS),
                    )
                blocks.append(block)
            keep(mid_table, tile, blocks)
        for tile in range(shifts // per_edge):
            blocks = []
            for k in range(rows // 8):
                block = None
                for q in range(per_edge):
                    b, start = tile * per_edge + q, q * edge_span
                    upper = moved(b, k, start)
                    lower = moved(b, k, start - rows)
                    piece = jnp.where(lane8 < start + EDGE_ROWS, upper, lower)
                    block = piece if block is None else jnp.where(lane8 < start, block, piece)
                blocks.append(block)
            keep(edge_table, tile, blocks)

    def part(source, table, which):
        depth = source.shape[0]
        group = DEPTH // depth
        both = jnp.zeros((2 * rows, cols), jnp.float32)
        rest = jnp.zeros((rows, cols), jnp.float32)
        for first in range(0, shifts, group):
            highs, lows = [], []
            for b in range(first, first + group):
                offset = EDGE_COLS - half + min(b, width - 1)
                high, low = split(pltpu.roll(source, wide - offset, axis=1)[:, 0:cols])
                highs.append(high)
                lows.append(low)
            block = table[which, :, first * depth : (first + group) * depth]
            both = both + jnp.dot(
                block, jnp.concatenate(highs, axis=0), preferred_element_type=jnp.float32
            )
            rest = rest + jnp.dot(
                block[0:rows], jnp.concatenate(lows, axis=0), preferred_element_type=jnp.float32
            )
        return both[0:rows] + (both[rows:] + rest)

    def correlate(phase, which):
        receive(phase, SIDES)
        middle = part(ext[phase, mid_r, :], mid_table, which)
        receive(phase, OTHERS)
        edges = jnp.concatenate(
            [ext[phase, 0:EDGE_ROWS, :], ext[phase, EDGE_ROWS + rows : tall, :]], axis=0
        )
        return middle + part(edges, edge_table, which)

    def laplacian(phase):
        center = ext[phase, mid_r, mid_c]
        upper = ext[phase, pl.ds(EDGE_ROWS - 1, rows), mid_c]
        lower = ext[phase, pl.ds(EDGE_ROWS + 1, rows), mid_c]
        band = ext[phase, mid_r, :]
        left = pltpu.roll(band, 1, axis=1)[:, EDGE_COLS : EDGE_COLS + cols]
        right = pltpu.roll(band, wide - 1, axis=1)[:, EDGE_COLS : EDGE_COLS + cols]
        return 4.0 * center - upper - lower - left - right

    def operate(phase, slot=None):
        blurred = correlate(phase, 0)
        put(phase + 1, blurred)
        smooth = PENALTY * laplacian(phase)
        if slot is not None:
            center = ext[phase, mid_r, mid_c]
            spread(slot, center * center, blurred * blurred + center * smooth)
        return correlate(phase + 1, 1) + smooth

    def put(phase, value):
        ext[phase, mid_r, mid_c] = value
        send(phase)

    lane = lane8[0:1]

    def fold(x):
        line = jnp.sum(x, axis=0, keepdims=True)
        line = functools.reduce(
            jnp.add, [line[:, k : k + 128] for k in range(0, line.shape[1], 128)]
        )
        return line + pltpu.roll(line, 64, axis=1)

    def spread(slot, norms, products):
        red[slot, me] = jnp.where(lane < 64, fold(norms), fold(products))
        others(
            lambda place: pltpu.make_async_remote_copy(
                src_ref=red.at[slot, me],
                dst_ref=red.at[slot, me],
                send_sem=red_send.at[slot],
                recv_sem=red_recv.at[slot],
                device_id=place,
                device_id_type=MESH,
            ).start()
        )

    def all_slots(slot):
        return pltpu.make_async_remote_copy(
            src_ref=red.at[slot, pl.ds(0, count - 1)],
            dst_ref=red.at[slot, pl.ds(0, count - 1)],
            send_sem=red_send.at[slot],
            recv_sem=red_recv.at[slot],
            device_id=(row, col),
            device_id_type=MESH,
        )

    def gather(slot):
        all_slots(slot).wait_recv()
        line = jnp.sum(red[slot], axis=0)
        norm = jnp.sum(jnp.where(lane < 64, line, 0.0), axis=1, keepdims=True)
        product = jnp.sum(jnp.where(lane < 64, 0.0, line), axis=1, keepdims=True)
        return norm, product

    pl.semaphore_wait(barrier, count - 1)
    send(0)
    build(0)
    build(1)

    template = guess_ref[...]
    residual = right_ref[...] - operate(0)
    norm_last = step_size = direction = along = None
    for iteration in range(ITERS):
        put(2 * iteration + 2, residual)
        applied = operate(2 * iteration + 2, iteration)
        norm, product = gather(iteration)
        if iteration == 0:
            step_size = norm / product
            direction, along = residual, applied
        else:
            ratio = norm / norm_last
            step_size = norm / (product - ratio * norm / step_size)
            direction = residual + ratio * direction
            along = applied + ratio * along
        norm_last = norm
        template = template + step_size * direction
        residual = residual - step_size * along

    template_ref[...] = template
    residual_ref[...] = residual
    for phase in range(phases):
        finish(phase)
    for slot in range(ITERS):
        all_slots(slot).wait_send()


def on_device(n_row, n_col, right_side, initial_guess, kernel):
    rows, cols = right_side.shape
    tall = rows + 2 * EDGE_ROWS
    group = DEPTH // (2 * EDGE_ROWS)
    shifts = -(-kernel.shape[0] // group) * group
    phases, count = 2 * (ITERS + 1), n_row * n_col
    shape = jax.ShapeDtypeStruct((rows, cols), jnp.float32)
    vmem = pl.BlockSpec(memory_space=pltpu.VMEM)
    return pl.pallas_call(
        functools.partial(body, n_row, n_col),
        out_shape=(shape, shape),
        in_specs=[vmem] * 3,
        out_specs=(vmem, vmem),
        scratch_shapes=[
            pltpu.VMEM((phases, tall, cols + 2 * EDGE_COLS), jnp.float32),
            pltpu.VMEM((2, 2 * rows, shifts * rows), jnp.bfloat16),
            pltpu.VMEM((2, 2 * rows, shifts * 2 * EDGE_ROWS), jnp.bfloat16),
            pltpu.VMEM((ITERS, count, 1, 128), jnp.float32),
            pltpu.SemaphoreType.DMA((phases, len(DIRECTIONS))),
            pltpu.SemaphoreType.DMA((phases, len(DIRECTIONS))),
            pltpu.SemaphoreType.DMA((ITERS,)),
            pltpu.SemaphoreType.DMA((ITERS,)),
        ],
        compiler_params=pltpu.CompilerParams(collective_id=0, has_side_effects=True),
    )(right_side, initial_guess, kernel)


def solution(mesh):
    placed = (P("row", "col"), P("row", "col"), P())
    return jax.shard_map(
        functools.partial(on_device, mesh.shape["row"], mesh.shape["col"]),
        mesh=mesh,
        in_specs=placed,
        out_specs=(P("row", "col"), P("row", "col")),
        check_vma=False,
    )
```

```python
import functools

import jax
import jax.numpy as jnp
from jax import lax
from jax.experimental import pallas as pl
from jax.experimental.pallas import tpu as pltpu
from jax.sharding import PartitionSpec as P

ITERS = 3
PENALTY = 0.05
EDGE_ROWS = 16
EDGE_COLS = 128
DEPTH = 512
LANES = 128
MESH = pl.DeviceIdType.MESH
DIRECTIONS = ((-1, -1), (-1, 1), (1, -1), (1, 1), (0, -1), (0, 1), (-1, 0), (1, 0))
SIDES = (4, 5)
OTHERS = (0, 1, 2, 3, 6, 7)


def span(step, size, edge):
    if step > 0:
        return size, 0, edge
    if step < 0:
        return edge, size + edge, edge
    return edge, edge, size


def split(x):
    high = x.astype(jnp.bfloat16)
    low = (x - high.astype(jnp.float32)).astype(jnp.bfloat16)
    return high, low


def body(
    n_row, n_col,
    right_ref, guess_ref, kernel_ref, template_ref, residual_ref,
    ext, taps_ref, mid_table, edge_table, got, smooth_ref, along_ref, direction_ref, last_ref,
    red, send_sem, recv_sem, red_send, red_recv,
):
    rows, cols = right_ref.shape
    row, col = lax.axis_index("row"), lax.axis_index("col")
    me, count = row * n_col + col, n_row * n_col
    tall, wide = rows + 2 * EDGE_ROWS, cols + 2 * EDGE_COLS
    width = kernel_ref.shape[0]
    half = width // 2
    shifts = mid_table.shape[1] * LANES // rows
    mid_r, mid_c = pl.ds(EDGE_ROWS, rows), pl.ds(EDGE_COLS, cols)

    barrier = pltpu.get_barrier_semaphore()

    def others(act):
        def along_row(r, carry):
            def one(c, inner):
                pl.when(r * n_col + c != me)(lambda: act((r, c)))
                return inner

            return lax.fori_loop(0, n_col, one, carry)

        lax.fori_loop(0, n_row, along_row, 0)

    others(
        lambda place: pl.semaphore_signal(barrier, inc=1, device_id=place, device_id_type=MESH)
    )

    phases = ext.shape[0]
    ext[0, mid_r, mid_c] = guess_ref[...]

    @pl.when(row == 0)
    def _():
        ext[:, 0:EDGE_ROWS, :] = jnp.zeros((phases, EDGE_ROWS, wide), jnp.float32)

    @pl.when(row == n_row - 1)
    def _():
        ext[:, EDGE_ROWS + rows : tall, :] = jnp.zeros((phases, EDGE_ROWS, wide), jnp.float32)

    @pl.when(col == 0)
    def _():
        ext[:, :, 0:EDGE_COLS] = jnp.zeros((phases, tall, EDGE_COLS), jnp.float32)

    @pl.when(col == n_col - 1)
    def _():
        ext[:, :, EDGE_COLS + cols : wide] = jnp.zeros((phases, tall, EDGE_COLS), jnp.float32)

    def inside(dr, dc):
        checks = []
        if dr:
            checks.append(row + dr >= 0 if dr < 0 else row + dr < n_row)
        if dc:
            checks.append(col + dc >= 0 if dc < 0 else col + dc < n_col)
        return functools.reduce(jnp.logical_and, checks)

    def strip(phase, index):
        dr, dc = DIRECTIONS[index]
        r_src, r_dst, r_len = span(dr, rows, EDGE_ROWS)
        c_src, c_dst, c_len = span(dc, cols, EDGE_COLS)
        return pltpu.make_async_remote_copy(
            src_ref=ext.at[phase, pl.ds(r_src, r_len), pl.ds(c_src, c_len)],
            dst_ref=ext.at[phase, pl.ds(r_dst, r_len), pl.ds(c_dst, c_len)],
            send_sem=send_sem.at[phase, index],
            recv_sem=recv_sem.at[phase, index],
            device_id=(row + dr, col + dc),
            device_id_type=MESH,
        )

    def send(phase):
        for index, (dr, dc) in enumerate(DIRECTIONS):
            pl.when(inside(dr, dc))(lambda index=index: strip(phase, index).start())

    def receive(phase, which):
        for index in which:
            dr, dc = DIRECTIONS[index]
            pl.when(inside(-dr, -dc))(lambda index=index: strip(phase, index).wait_recv())

    def finish(phase):
        for index, (dr, dc) in enumerate(DIRECTIONS):
            pl.when(inside(dr, dc))(lambda index=index: strip(phase, index).wait_send())

    sub = lax.broadcasted_iota(jnp.int32, (8, LANES), 0)
    lane8 = lax.broadcasted_iota(jnp.int32, (8, LANES), 1)
    per_mid, edge_span = LANES // rows, 2 * EDGE_ROWS
    per_edge = LANES // edge_span

    def flip(x):
        return jnp.concatenate([x[a : a + 1] for a in reversed(range(width))] + [x[width:]], axis=0)

    def prepare():
        taps = kernel_ref[...]
        taps = jnp.concatenate([taps, jnp.zeros((width, LANES - width), jnp.float32)], axis=1)
        taps = jnp.concatenate([taps, jnp.zeros((LANES - width, LANES), jnp.float32)], axis=0)
        taps_ref[0] = taps.T
        taps_ref[1] = flip(flip(taps).T)

    def build(which, quad):
        bands = []
        for q in range(per_edge):
            line = taps_ref[which, pl.ds(quad * per_edge + q, 1), :]
            eight = pltpu.roll(jnp.broadcast_to(line, (8, LANES)), EDGE_ROWS - half, axis=1)
            for bit in (1, 2, 4):
                eight = jnp.where((sub & bit) != 0, pltpu.roll(eight, bit, axis=1), eight)
            bands.append(eight)

        def moved(q, k, shift):
            return pltpu.roll(bands[q], (8 * k + shift) % LANES, axis=1)

        def keep(table, tile, blocks):
            high, low = split(jnp.concatenate(blocks, axis=0))
            table[which, tile, 0:rows, :] = high
            table[which, tile, rows : 2 * rows, :] = low

        for t in range(per_edge // per_mid):
            blocks = []
            for k in range(rows // 8):
                block = moved(t * per_mid, k, -EDGE_ROWS)
                for q in range(1, per_mid):
                    other = moved(t * per_mid + q, k, q * rows - EDGE_ROWS)
                    block = jnp.where(lane8 < q * rows, block, other)
                blocks.append(block)
            keep(mid_table, quad * (per_edge // per_mid) + t, blocks)
        blocks = []
        for k in range(rows // 8):
            block = None
            for q in range(per_edge):
                start = q * edge_span
                upper = moved(q, k, start)
                lower = moved(q, k, start - rows)
                piece = jnp.where(lane8 < start + EDGE_ROWS, upper, lower)
                block = piece if block is None else jnp.where(lane8 < start, block, piece)
            blocks.append(block)
        keep(edge_table, quad, blocks)

    def build_half(which):
        def inner(quad, c):
            build(which, quad)
            return c

        lax.fori_loop(0, shifts // per_edge, inner, 0)

    def part(source, table, which):
        depth = source.shape[0]
        group = DEPTH // depth
        both = jnp.zeros((2 * rows, cols), jnp.float32)
        rest = jnp.zeros((rows, cols), jnp.float32)
        for first in range(0, shifts, group):
            highs, lows = [], []
            for b in range(first, first + group):
                offset = EDGE_COLS - half + min(b, width - 1)
                high, low = split(pltpu.roll(source, wide - offset, axis=1)[:, 0:cols])
                highs.append(high)
                lows.append(low)
            tiles = range(first * depth // LANES, (first + group) * depth // LANES)
            block = jnp.concatenate([table[which, t] for t in tiles], axis=1)
            both = both + jnp.dot(
                block, jnp.concatenate(highs, axis=0), preferred_element_type=jnp.float32
            )
            rest = rest + jnp.dot(
                block[0:rows], jnp.concatenate(lows, axis=0), preferred_element_type=jnp.float32
            )
        return both[0:rows] + (both[rows:] + rest)

    def correlate(phase, which):
        receive(phase, SIDES)
        middle = part(ext[phase, mid_r, :], mid_table, which)
        receive(phase, OTHERS)
        edges = jnp.concatenate(
            [ext[phase, 0:EDGE_ROWS, :], ext[phase, EDGE_ROWS + rows : tall, :]], axis=0
        )
        return middle + part(edges, edge_table, which)

    def laplacian(phase):
        center = ext[phase, mid_r, mid_c]
        upper = ext[phase, pl.ds(EDGE_ROWS - 1, rows), mid_c]
        lower = ext[phase, pl.ds(EDGE_ROWS + 1, rows), mid_c]
        band = ext[phase, mid_r, :]
        left = pltpu.roll(band, 1, axis=1)[:, EDGE_COLS : EDGE_COLS + cols]
        right = pltpu.roll(band, wide - 1, axis=1)[:, EDGE_COLS : EDGE_COLS + cols]
        return 4.0 * center - upper - lower - left - right

    def put(phase, value):
        ext[phase, mid_r, mid_c] = value
        send(phase)

    lane = lane8[0:1]

    def fold(x):
        line = jnp.sum(x, axis=0, keepdims=True)
        line = functools.reduce(
            jnp.add, [line[:, k : k + 128] for k in range(0, line.shape[1], 128)]
        )
        return line + pltpu.roll(line, 64, axis=1)

    def spread(slot, norms, products):
        red[slot, me] = jnp.where(lane < 64, fold(norms), fold(products))
        others(
            lambda place: pltpu.make_async_remote_copy(
                src_ref=red.at[slot, me],
                dst_ref=red.at[slot, me],
                send_sem=red_send.at[slot],
                recv_sem=red_recv.at[slot],
                device_id=place,
                device_id_type=MESH,
            ).start()
        )

    def all_slots(slot):
        return pltpu.make_async_remote_copy(
            src_ref=red.at[slot, pl.ds(0, count - 1)],
            dst_ref=red.at[slot, pl.ds(0, count - 1)],
            send_sem=red_send.at[slot],
            recv_sem=red_recv.at[slot],
            device_id=(row, col),
            device_id_type=MESH,
        )

    def gather(slot):
        all_slots(slot).wait_recv()
        line = jnp.sum(red[slot], axis=0)
        norm = jnp.sum(jnp.where(lane < 64, line, 0.0), axis=1, keepdims=True)
        product = jnp.sum(jnp.where(lane < 64, 0.0, line), axis=1, keepdims=True)
        return norm, product

    template_ref[...] = guess_ref[...]
    along_ref[...] = jnp.zeros_like(along_ref)
    direction_ref[...] = jnp.zeros_like(direction_ref)
    last_ref[...] = jnp.ones_like(last_ref)
    prepare()
    build_half(0)
    pl.semaphore_wait(barrier, count - 1)
    send(0)
    build_half(1)

    def update(slot):
        applied = got[...] + smooth_ref[...]
        residual = residual_ref[...]
        norm, product = gather(slot)
        norm_last, step_last = last_ref[0:1, 0:1], last_ref[1:2, 0:1]
        ratio = jnp.where(slot > 0, norm / norm_last, 0.0)
        step_size = norm / (product - ratio * norm / step_last)
        direction = residual + ratio * direction_ref[...]
        along = applied + ratio * along_ref[...]
        direction_ref[...], along_ref[...] = direction, along
        last_ref[0:1, :] = jnp.broadcast_to(norm, (1, LANES))
        last_ref[1:2, :] = jnp.broadcast_to(step_size, (1, LANES))
        template_ref[...] = template_ref[...] + step_size * direction
        residual_ref[...] = residual - step_size * along

    def advance(phase, carry):
        which, slot = lax.rem(phase, 2), phase // 2 - 1
        got[...] = correlate(phase, which)

        @pl.when(which == 0)
        def _():
            put(phase + 1, got[...])
            smooth = PENALTY * laplacian(phase)
            smooth_ref[...] = smooth

            @pl.when(slot >= 0)
            def _():
                blurred, center = got[...], ext[phase, mid_r, mid_c]
                spread(slot, center * center, blurred * blurred + center * smooth_ref[...])

        @pl.when(which == 1)
        def _():
            @pl.when(slot < 0)
            def _():
                residual_ref[...] = right_ref[...] - (got[...] + smooth_ref[...])

            @pl.when(slot >= 0)
            def _():
                update(slot)

            @pl.when(phase < phases - 1)
            def _():
                put(phase + 1, residual_ref[...])

            @pl.when(slot >= 0)
            def _():
                all_slots(slot).wait_send()

        finish(phase)
        return carry

    lax.fori_loop(0, phases, advance, 0)


def on_device(n_row, n_col, right_side, initial_guess, kernel):
    rows, cols = right_side.shape
    tall = rows + 2 * EDGE_ROWS
    group = DEPTH // (2 * EDGE_ROWS)
    shifts = -(-kernel.shape[0] // group) * group
    phases, count = 2 * (ITERS + 1), n_row * n_col
    shape = jax.ShapeDtypeStruct((rows, cols), jnp.float32)
    vmem = pl.BlockSpec(memory_space=pltpu.VMEM)
    return pl.pallas_call(
        functools.partial(body, n_row, n_col),
        out_shape=(shape, shape),
        in_specs=[vmem] * 3,
        out_specs=(vmem, vmem),
        scratch_shapes=[
            pltpu.VMEM((phases, tall, cols + 2 * EDGE_COLS), jnp.float32),
            pltpu.VMEM((2, LANES, LANES), jnp.float32),
            pltpu.VMEM((2, shifts * rows // LANES, 2 * rows, LANES), jnp.bfloat16),
            pltpu.VMEM((2, shifts * 2 * EDGE_ROWS // LANES, 2 * rows, LANES), jnp.bfloat16),
            pltpu.VMEM((rows, cols), jnp.float32),
            pltpu.VMEM((rows, cols), jnp.float32),
            pltpu.VMEM((rows, cols), jnp.float32),
            pltpu.VMEM((rows, cols), jnp.float32),
            pltpu.VMEM((8, LANES), jnp.float32),
            pltpu.VMEM((ITERS, count, 1, 128), jnp.float32),
            pltpu.SemaphoreType.DMA((phases, len(DIRECTIONS))),
            pltpu.SemaphoreType.DMA((phases, len(DIRECTIONS))),
            pltpu.SemaphoreType.DMA((ITERS,)),
            pltpu.SemaphoreType.DMA((ITERS,)),
        ],
        compiler_params=pltpu.CompilerParams(collective_id=0, has_side_effects=True),
    )(right_side, initial_guess, kernel)


def solution(mesh):
    placed = (P("row", "col"), P("row", "col"), P())
    return jax.shard_map(
        functools.partial(on_device, mesh.shape["row"], mesh.shape["col"]),
        mesh=mesh,
        in_specs=placed,
        out_specs=(P("row", "col"), P("row", "col")),
        check_vma=False,
    )
```
